128 devices in a mesh: data: 1, branch: 128 (over z, y, x, core).
Axes of the slice: x: 4, y: 4, z: 4, core: 2. Of those that a mesh axis runs over, the one named last changes fastest.
Arguments:
- x: bfloat16 [1, 1024, 3072], P('data', 'branch')
- h: bfloat16 [1, 1024, 3072], P('data', 'branch')
- in_qkv: bfloat16 [2, 1, 3072, 9216], replicated
- in_proj: bfloat16 [2, 1, 24, 128, 3072], replicated
- in_up: bfloat16 [2, 1, 3072, 12288], replicated
- in_down: bfloat16 [2, 1, 12288, 3072], replicated
- tail_qkv: bfloat16 [1, 3072, 9216], replicated
- tail_proj: bfloat16 [1, 24, 128, 3072], replicated
- tail_up: bfloat16 [1, 3072, 12288], replicated
- tail_down: bfloat16 [1, 12288, 3072], replicated
- z_hint: bfloat16 [3072, 3072], replicated
- z_out: bfloat16 [1, 3072, 3072], replicated
- w_final: bfloat16 [3072, 3072], replicated
Outputs:
- output: bfloat16 [1, 1024, 3072], P('data', 'branch')
All inputs are finite; a program needn't handle non-finite values.
Results may differ from the reference program's by a relative error of at most 0.019224.
Values are sent between devices in bfloat16 or wider.
A program may use at most 1.5 GiB of HBM per device.

```python
import math
import jax
import jax.numpy as jnp
from jax import lax

DIM = 3072
HEADS = 24
HEAD_DIM = 128
TOKENS = 1024
CTRL = 1
TAIL = 1
Q_BLOCK = 256
LN_EPS = 1e-6
ATTN_SCALE = HEAD_DIM ** -0.5
SHARPNESS = math.sqrt(math.log(TOKENS / 8.0))


def draw_normal(rng_key, out_shape, std_scale):
    return jax.random.normal(rng_key, out_shape, jnp.float32) * std_scale


def draw_qkv(rng_key, lead_dims):
    qk_gain = math.sqrt(SHARPNESS)
    section_gain = jnp.array([qk_gain, qk_gain, 1.0], jnp.float32).reshape(3, 1)
    raw_qkv = draw_normal(rng_key, lead_dims + (DIM, 3, DIM), DIM ** -0.5) * section_gain
    return raw_qkv.reshape(lead_dims + (DIM, 3 * DIM)).astype(jnp.bfloat16)


def setup_inputs(seed: int = 0, part: int = 0) -> dict:
    root_key = jax.random.key(seed)
    part_key = jax.random.fold_in(root_key, part)
    key_x, key_h = jax.random.split(part_key, 2)
    weight_keys = jax.random.split(root_key, 11)
    head_lead = (2, CTRL)
    tail_lead = (TAIL,)
    return {
        'x': draw_normal(key_x, (1, TOKENS, DIM), 1.0).astype(jnp.bfloat16),
        'h': draw_normal(key_h, (1, TOKENS, DIM), 1.0).astype(jnp.bfloat16),
        'in_qkv': draw_qkv(weight_keys[0], head_lead),
        'in_proj': draw_normal(weight_keys[1], head_lead + (HEADS, HEAD_DIM, DIM), DIM ** -0.5).astype(jnp.bfloat16),
        'in_up': draw_normal(weight_keys[2], head_lead + (DIM, 4 * DIM), DIM ** -0.5).astype(jnp.bfloat16),
        'in_down': draw_normal(weight_keys[3], head_lead + (4 * DIM, DIM), (4 * DIM) ** -0.5).astype(jnp.bfloat16),
        'tail_qkv': draw_qkv(weight_keys[4], tail_lead),
        'tail_proj': draw_normal(weight_keys[5], tail_lead + (HEADS, HEAD_DIM, DIM), DIM ** -0.5).astype(jnp.bfloat16),
        'tail_up': draw_normal(weight_keys[6], tail_lead + (DIM, 4 * DIM), DIM ** -0.5).astype(jnp.bfloat16),
        'tail_down': draw_normal(weight_keys[7], tail_lead + (4 * DIM, DIM), (4 * DIM) ** -0.5).astype(jnp.bfloat16),
        'z_hint': draw_normal(weight_keys[8], (DIM, DIM), DIM ** -0.5).astype(jnp.bfloat16),
        'z_out': draw_normal(weight_keys[9], (CTRL, DIM, DIM), 0.6 * DIM ** -0.5).astype(jnp.bfloat16),
        'w_final': draw_normal(weight_keys[10], (DIM, DIM), DIM ** -0.5).astype(jnp.bfloat16),
    }


def layer_norm(residual):
    residual_f32 = residual.astype(jnp.float32)
    centred = residual_f32 - jnp.mean(residual_f32, axis=-1, keepdims=True)
    variance = jnp.mean(centred * centred, axis=-1, keepdims=True)
    return (centred * lax.rsqrt(variance + LN_EPS)).astype(jnp.bfloat16)


def attention(normed, w_qkv, w_proj):
    qkv_rows = jnp.dot(normed, w_qkv, preferred_element_type=jnp.float32).astype(jnp.bfloat16).reshape(TOKENS, 3, HEADS, HEAD_DIM)
    key_rows = qkv_rows[:, 1].astype(jnp.float32)
    value_rows = qkv_rows[:, 2].astype(jnp.float32)
    query_blocks = qkv_rows[:, 0].reshape(TOKENS // Q_BLOCK, Q_BLOCK, HEADS, HEAD_DIM)

    def one_block(query_rows):
        scores = jnp.einsum('qhe,khe->hqk', query_rows.astype(jnp.float32), key_rows) * ATTN_SCALE
        attn_probs = jax.nn.softmax(scores, axis=-1).astype(jnp.bfloat16)
        return jnp.einsum('hqk,khe->qhe', attn_probs.astype(jnp.float32), value_rows).astype(jnp.bfloat16)

    attn_out = lax.map(one_block, query_blocks).reshape(TOKENS, HEADS, HEAD_DIM)
    return jnp.einsum('qhe,hed->qd', attn_out.astype(jnp.float32), w_proj.astype(jnp.float32)).astype(jnp.bfloat16)


def transformer_block(residual, w_qkv, w_proj, w_up, w_down):
    proj_out = attention(layer_norm(residual), w_qkv, w_proj)
    residual = (residual.astype(jnp.float32) + proj_out.astype(jnp.float32)).astype(jnp.bfloat16)
    hidden = jax.nn.gelu(jnp.dot(layer_norm(residual), w_up, preferred_element_type=jnp.float32), approximate=True).astype(jnp.bfloat16)
    mlp_out = jnp.dot(hidden, w_down, preferred_element_type=jnp.float32).astype(jnp.bfloat16)
    return (residual.astype(jnp.float32) + mlp_out.astype(jnp.float32)).astype(jnp.bfloat16)


def reference(x, h, in_qkv, in_proj, in_up, in_down, tail_qkv, tail_proj, tail_up, tail_down, z_hint, z_out, w_final):
    base_state = x[0]
    hint_proj = jnp.dot(h[0], z_hint, preferred_element_type=jnp.float32).astype(jnp.bfloat16)
    ctrl_state = (base_state.astype(jnp.float32) + hint_proj.astype(jnp.float32)).astype(jnp.bfloat16)

    def ctrl_step(scan_carry, layer_weights):
        base_prev, ctrl_prev = scan_carry
        stack_qkv, stack_proj, stack_up, stack_down, z_layer = layer_weights
        base_out = transformer_block(base_prev, stack_qkv[0], stack_proj[0], stack_up[0], stack_down[0])
        ctrl_next = transformer_block(ctrl_prev, stack_qkv[1], stack_proj[1], stack_up[1], stack_down[1])
        ctrl_resid = jnp.dot(ctrl_next, z_layer, preferred_element_type=jnp.float32).astype(jnp.bfloat16)
        base_next = (base_out.astype(jnp.float32) + ctrl_resid.astype(jnp.float32)).astype(jnp.bfloat16)
        return (base_next, ctrl_next), None

    head_weights = (jnp.swapaxes(in_qkv, 0, 1), jnp.swapaxes(in_proj, 0, 1), jnp.swapaxes(in_up, 0, 1), jnp.swapaxes(in_down, 0, 1), z_out)
    head_carry, unused_ys = lax.scan(ctrl_step, (base_state, ctrl_state), head_weights)

    def tail_step(base_prev, layer_weights):
        return transformer_block(base_prev, layer_weights[0], layer_weights[1], layer_weights[2], layer_weights[3]), None

    tail_state, unused_tail = lax.scan(tail_step, head_carry[0], (tail_qkv, tail_proj, tail_up, tail_down))
    return jnp.dot(layer_norm(tail_state), w_final, preferred_element_type=jnp.float32).astype(jnp.bfloat16)[None]
```

```python
import functools

import jax
import jax.numpy as jnp
from jax import lax
from jax.experimental import pallas as pl
from jax.experimental.pallas import tpu as pltpu
from jax.sharding import PartitionSpec as P

MESH = pl.DeviceIdType.MESH
F32 = jnp.float32
BF16 = jnp.bfloat16
LN_EPS = 1e-6
W = 8
HD = 128
SLOTS = 17

PH_XH, PH_C0, PH_O, PH_U, PH_C1, PH_A1, PH_OT, PH_UT, PH_A2 = 0, 1, 2, 4, 6, 7, 8, 9, 10
NUM_PH = 11
PH_ATT = (PH_O, PH_O + 1, PH_OT)
PH_MID = (PH_U, PH_U + 1, PH_UT)


def normalise(rows):
    centred = rows - jnp.mean(rows, axis=-1, keepdims=True)
    variance = jnp.mean(centred * centred, axis=-1, keepdims=True)
    return (centred * lax.rsqrt(variance + LN_EPS)).astype(BF16)


def add_rounded(a, b):
    return (a.astype(F32) + b.astype(F32)).astype(BF16)


def kernel(n, heads_w, x_ref, h_ref, in_qkv, in_proj, in_up, in_down, tail_qkv, tail_proj, tail_up, tail_down, z_hint, z_out, w_final,
           y_ref, wbuf, wsem, xs, xh, gathered, lnbuf, hid, qkv_out, qkv_in, o_out, part_out, part_in, sum_out, sum_in, sum_own, ystage, ybuf,
           ag_send, ag_recv, qkv_send, qkv_recv, o_send, o_recv, part_send, part_recv, sum_send, sum_recv, y_send, y_recv):
    T = n // W
    R = x_ref.shape[0]
    D = x_ref.shape[1]
    M = W * R
    C = D // W
    FS = hid.shape[1]
    NW1 = FS // C
    scale = HD ** -0.5

    me = lax.axis_index('branch')
    if n == 128:
        c = lax.rem(me, 2)
        x0 = lax.rem(me // 2, 2)
        x1 = lax.rem(me // 4, 2)
        y0 = lax.rem(me // 8, 2)
        y1 = lax.rem(me // 16, 2)
        j = y0 * 2 + x0
        t = (me // 32) * 4 + y1 * 2 + x1
        spread = T // 2
    else:
        c = lax.rem(me, 2)
        j = lax.rem(me, W) // 2
        t = me // W
        spread = 0
    w = j * 2 + c

    def dev(tt, jj, cc):
        if n == 128:
            return (tt // 4) * 32 + lax.rem(tt // 2, 2) * 16 + (jj // 2) * 8 + lax.rem(tt, 2) * 4 + lax.rem(jj, 2) * 2 + cc
        return tt * W + jj * 2 + cc

    def near(r):
        return lax.rem(j // 2 + r // 2, 2) * 2 + lax.rem(lax.rem(j, 2) + lax.rem(r, 2), 2)

    def rcopy(src, dst, ssem, rsem, device):
        return pltpu.make_async_remote_copy(src_ref=src, dst_ref=dst, send_sem=ssem, recv_sem=rsem, device_id={'branch': device}, device_id_type=MESH)

    partner = dev(t, j, 1 - c)

    def cols(ww):
        return pl.ds(pl.multiple_of(ww * C, HD), C)

    chunks = []

    def add(*pieces):
        chunks.append(pieces)
        return len(chunks) - 1

    def columns_of(ref, start):
        return ref.at[:, pl.ds(pl.multiple_of(start, HD), C)]

    def add_qkv(ref):
        return [add(columns_of(ref, p * D + w * C)) for p in (1, 2, 0)][0]

    def add_up(ref):
        return [add(columns_of(ref, w * FS + i * C)) for i in range(NW1)][0]

    def add_down(ref):
        first = len(chunks)
        for core in (1 - c, c):
            for pair in ((1, 2), (3, 0)):
                add(*[ref.at[pl.ds(pl.multiple_of(w * FS, 16), FS), cols(near(r) * 2 + core)] for r in pair])
        return first

    qkv_refs = (in_qkv.at[0], in_qkv.at[1], tail_qkv.at[0])
    proj_refs = (in_proj.at[0], in_proj.at[1], tail_proj.at[0])
    up_refs = (in_up.at[0], in_up.at[1], tail_up.at[0])
    down_refs = (in_down.at[0], in_down.at[1], tail_down.at[0])
    k_hint = add(columns_of(z_hint, w * C))
    k_qkv, k_proj, k_up, k_down = {}, {}, {}, {}
    for b in (0, 1):
        k_qkv[b] = add_qkv(qkv_refs[b])
    for b in (0, 1):
        k_proj[b] = add(columns_of(proj_refs[b], w * C))
    for b in (1, 0):
        k_up[b] = add_up(up_refs[b])
        k_down[b] = add_down(down_refs[b])
    k_zout = add(columns_of(z_out.at[0], w * C))
    k_qkv[2] = add_qkv(qkv_refs[2])
    k_proj[2] = add(columns_of(proj_refs[2], w * C))
    k_up[2] = add_up(up_refs[2])
    k_down[2] = add_down(down_refs[2])
    k_final = add(columns_of(w_final, w * C))

    def fetch(k):
        slot = k % SLOTS
        if len(chunks[k]) == 1:
            pltpu.make_async_copy(chunks[k][0], wbuf.at[slot], wsem.at[slot]).start()
        else:
            for i, piece in enumerate(chunks[k]):
                pltpu.make_async_copy(piece, wbuf.at[slot, pl.ds(i * FS, FS)], wsem.at[slot]).start()

    def ready(slot):
        pltpu.make_async_copy(columns_of(z_hint, 0), wbuf.at[slot], wsem.at[slot]).wait()

    def refill(first, count):
        for k in range(first, first + count):
            if k + SLOTS < len(chunks):
                fetch(k + SLOTS)

    for k in range(min(SLOTS, len(chunks))):
        fetch(k)

    barrier = pltpu.get_barrier_semaphore()

    def greet_group(ww, carry):
        @pl.when(ww != w)
        def _():
            pl.semaphore_signal(barrier, inc=1, device_id={'branch': dev(t, ww // 2, lax.rem(ww, 2))}, device_id_type=MESH)
        return carry

    def greet_tokens(tt, carry):
        @pl.when(tt != t)
        def _():
            pl.semaphore_signal(barrier, inc=1, device_id={'branch': dev(tt, j, c)}, device_id_type=MESH)
        return carry

    lax.fori_loop(0, W, greet_group, 0)
    lax.fori_loop(0, T, greet_tokens, 0)
    xs[w, 0] = x_ref[...]
    xs[w, 1] = h_ref[...]
    pl.semaphore_wait(barrier, W - 1 + T - 1)

    def piece(ph, jj, cc):
        if isinstance(ph, int) and ph == PH_XH:
            return xs.at[jj * 2 + cc]
        return gathered.at[ph - 1, :, cols(jj * 2 + cc)]

    def gather_start(ph):
        own = piece(ph, j, c)
        for r in (3, 1, 2):
            rcopy(own, own, ag_send.at[ph, r], ag_recv.at[ph, r], dev(t, near(r), c)).start()
        rcopy(own, own, ag_send.at[ph, 0], ag_recv.at[ph, 0], partner).start()

    def gather_forward(ph):
        for r in (1, 2, 3):
            got = piece(ph, near(r), c)
            rcopy(got, got, ag_send.at[ph, r], ag_recv.at[ph, r], partner).wait_recv()
            rcopy(got, got, ag_send.at[ph, 3 + r], ag_recv.at[ph, 3 + r], partner).start()

    def gather_finish(ph):
        for r in range(4):
            got = piece(ph, near(r), 1 - c)
            s = 0 if r == 0 else 3 + r
            rcopy(got, got, ag_send.at[ph, s], ag_recv.at[ph, s], partner).wait_recv()

    def gather_drain(ph):
        for s in range(7):
            own = piece(ph, j, c)
            rcopy(own, own, ag_send.at[ph, s], ag_recv.at[ph, s], partner).wait_send()

    def layer_norm(load):
        def rows16(i, carry):
            row = pl.ds(pl.multiple_of(i * 16, 16), 16)
            lnbuf[row, :] = normalise(load(row).astype(F32))
            return carry
        lax.fori_loop(0, M // 16, rows16, 0)

    def matmul(lhs, k):
        slot = k % SLOTS
        ready(slot)
        out = jnp.dot(lhs, wbuf[slot], preferred_element_type=F32)
        return out

    def owner(blk, h):
        return (blk % 2) * heads_w + h + spread * c

    def qkv_block(blk, stage):
        first = k_qkv[blk]

        def part_step(i, carry):
            p = lax.rem(i + 1, 3)
            slot = lax.rem(first + i, SLOTS)
            ready(slot)
            out = jnp.dot(lnbuf[...], wbuf[slot], preferred_element_type=F32).astype(BF16)
            dst_rows = pl.ds(pl.multiple_of(t * M, M), M)
            for h in range(heads_w):
                qkv_out[blk, p, h] = out[:, h * HD:(h + 1) * HD]
            for h in range(heads_w):
                to = owner(blk, h)

                @pl.when(to != t)
                def _():
                    rcopy(qkv_out.at[blk, p, h], qkv_in.at[stage, p, dst_rows], qkv_send.at[blk, p, h], qkv_recv.at[stage, t], dev(to, j, c)).start()

                @pl.when(to == t)
                def _():
                    qkv_in[stage, p, dst_rows, :] = out[:, h * HD:(h + 1) * HD]
            return carry

        lax.fori_loop(0, 3, part_step, 0)
        refill(first, 3)

    def qkv_drain(blk, stage):
        for p in range(3):
            for h in range(heads_w):
                @pl.when(owner(blk, h) != t)
                def _():
                    rcopy(qkv_out.at[blk, p, h], qkv_in.at[stage, p, pl.ds(0, M)], qkv_send.at[blk, p, h], qkv_recv.at[stage, t], partner).wait_send()

    QB = min(128, T * M)
    place = t - spread * c
    owns = (jnp.logical_and(place >= 0, place < 2 * heads_w), jnp.logical_and(place >= 0, place < heads_w))
    own_blk = place // heads_w
    own_head = lax.rem(place, heads_w)

    def attention(stage):
        ph = PH_O + own_blk if stage == 0 else PH_OT
        blk = own_blk if stage == 0 else 2

        @pl.when(owns[stage])
        def _():
            def arrive(tt, carry):
                @pl.when(tt != t)
                def _():
                    slab = qkv_in.at[stage, :, pl.ds(pl.multiple_of(tt * M, M), M)]
                    rcopy(slab, slab, o_send.at[stage, t], qkv_recv.at[stage, tt], partner).wait_recv()
                return carry

            lax.fori_loop(0, T, arrive, 0)

            def queries(i, carry):
                row = pl.ds(pl.multiple_of(i * QB, QB), QB)
                s = lax.dot_general(qkv_in[stage, 0, row, :], qkv_in[stage, 1], (((1,), (1,)), ((), ())), preferred_element_type=F32) * scale
                e = jnp.exp(s - jnp.max(s, axis=-1, keepdims=True))
                p = (e * (1.0 / jnp.sum(e, axis=-1, keepdims=True))).astype(BF16)
                o_out[stage, row, :] = jnp.dot(p, qkv_in[stage, 2], preferred_element_type=F32).astype(BF16)
                for q in range(QB // M):
                    tt = i * (QB // M) + q
                    mine = pl.ds(pl.multiple_of(tt * M, M), M)
                    dst = gathered.at[ph - 1, :, pl.ds(pl.multiple_of(w * C + own_head * HD, HD), HD)]

                    @pl.when(tt != t)
                    def _():
                        rcopy(o_out.at[stage, mine], dst, o_send.at[stage, tt], o_recv.at[blk, own_head], dev(tt, j, c)).start()

                    @pl.when(tt == t)
                    def _():
                        dst[...] = o_out[stage, mine, :]
                return carry

            lax.fori_loop(0, T * M // QB, queries, 0)

    def attention_drain(stage):
        @pl.when(owns[stage])
        def _():
            def left(tt, carry):
                @pl.when(tt != t)
                def _():
                    mine = o_out.at[stage, pl.ds(pl.multiple_of(tt * M, M), M)]
                    rcopy(mine, mine, o_send.at[stage, tt], o_recv.at[0, 0], partner).wait_send()
                return carry
            lax.fori_loop(0, T, left, 0)

    def attention_gather(blk):
        ph = PH_ATT[blk]
        for h in range(heads_w):
            @pl.when(owner(blk, h) != t)
            def _():
                got = gathered.at[ph - 1, :, pl.ds(pl.multiple_of(w * C + h * HD, HD), HD)]
                rcopy(got, got, o_send.at[0, t], o_recv.at[blk, h], partner).wait_recv()
        gather_start(ph)

    def own_cols(blk):
        if blk == 0:
            return xh[0, :, cols(w)]
        return gathered[(PH_C0 if blk == 1 else PH_A1) - 1, :, cols(w)]

    def proj_block(blk):
        ph = PH_ATT[blk]
        gather_forward(ph)
        gather_finish(ph)
        out = matmul(gathered[ph - 1], k_proj[blk]).astype(BF16)
        gathered[PH_MID[blk] - 1, :, cols(w)] = add_rounded(own_cols(blk), out)
        refill(k_proj[blk], 1)
        gather_start(PH_MID[blk])

    def mlp_block(blk):
        ph = PH_MID[blk]
        gather_forward(ph)
        gather_finish(ph)
        layer_norm(lambda row: gathered[ph - 1, row, :])

        def up_step(i, carry):
            slot = lax.rem(k_up[blk] + i, SLOTS)
            ready(slot)
            out = jnp.dot(lnbuf[...], wbuf[slot], preferred_element_type=F32)
            hid[:, pl.ds(pl.multiple_of(i * C, HD), C)] = jax.nn.gelu(out, approximate=True).astype(BF16)
            return carry

        lax.fori_loop(0, NW1, up_step, 0)
        refill(k_up[blk], NW1)

        def down(first, s):
            slot = lax.rem(first + s // 2, SLOTS)

            @pl.when(lax.rem(s, 2) == 0)
            def _():
                ready(slot)
            return jnp.dot(hid[...], wbuf[slot, pl.ds(pl.multiple_of(lax.rem(s, 2) * FS, 16), FS), :], preferred_element_type=F32)

        def for_partner(s, carry):
            part_out[blk, s] = down(k_down[blk], s)
            rcopy(part_out.at[blk, s], part_in.at[blk, s], part_send.at[blk, s], part_recv.at[blk, s], partner).start()
            return carry

        lax.fori_loop(0, 4, for_partner, 0)
        refill(k_down[blk], 2)

        def for_core(s, carry):
            out = down(k_down[blk] + 2, s)
            rcopy(part_out.at[blk, s], part_in.at[blk, s], part_send.at[blk, s], part_recv.at[blk, s], partner).wait_recv()
            out = out + part_in[blk, s]

            @pl.when(s < 3)
            def _():
                sum_out[blk, s] = out
                rcopy(sum_out.at[blk, s], sum_in.at[blk, s], sum_send.at[blk, s], sum_recv.at[blk, s], dev(t, near(s + 1), c)).start()

            @pl.when(s == 3)
            def _():
                sum_own[blk] = out
            return carry

        lax.fori_loop(0, 4, for_core, 0)
        refill(k_down[blk] + 2, 2)

    def mlp_finish(blk):
        total = sum_own[blk]
        for s in range(3):
            rcopy(sum_out.at[blk, s], sum_in.at[blk, s], sum_send.at[blk, s], sum_recv.at[blk, s], partner).wait_recv()
            total = total + sum_in[blk, s]
        return add_rounded(gathered[PH_MID[blk] - 1, :, cols(w)], total.astype(BF16))

    def mlp_drain(blk):
        for s in range(4):
            rcopy(part_out.at[blk, s], part_in.at[blk, s], part_send.at[blk, s], part_recv.at[blk, s], partner).wait_send()
        for s in range(3):
            rcopy(sum_out.at[blk, s], sum_in.at[blk, s], sum_send.at[blk, s], sum_recv.at[blk, s], partner).wait_send()

    gather_start(PH_XH)
    gather_forward(PH_XH)
    gather_finish(PH_XH)
    for which in range(2):
        for i in range(M // 16):
            pair = [xs[16 // R * i + q, which].astype(F32) for q in range(16 // R)]
            xh[which, i * 16:(i + 1) * 16, :] = jnp.concatenate(pair, axis=0).astype(BF16)

    hint = matmul(xh[1], k_hint).astype(BF16)
    refill(k_hint, 1)
    gathered[PH_C0 - 1, :, cols(w)] = add_rounded(xh[0, :, cols(w)], hint)
    gather_start(PH_C0)
    layer_norm(lambda row: xh[0, row, :])
    qkv_block(0, 0)
    gather_forward(PH_C0)
    gather_finish(PH_C0)
    layer_norm(lambda row: gathered[PH_C0 - 1, row, :])
    qkv_block(1, 0)
    attention(0)
    attention_gather(0)
    attention_gather(1)
    proj_block(0)
    proj_block(1)
    mlp_block(1)
    mlp_block(0)
    gathered[PH_C1 - 1, :, cols(w)] = mlp_finish(1)
    gather_start(PH_C1)
    base = mlp_finish(0)
    gather_forward(PH_C1)
    gather_finish(PH_C1)
    resid = matmul(gathered[PH_C1 - 1], k_zout).astype(BF16)
    refill(k_zout, 1)
    gathered[PH_A1 - 1, :, cols(w)] = add_rounded(base, resid)
    gather_start(PH_A1)
    gather_forward(PH_A1)
    gather_finish(PH_A1)
    layer_norm(lambda row: gathered[PH_A1 - 1, row, :])
    qkv_block(2, 1)
    attention(1)
    attention_gather(2)
    proj_block(2)
    mlp_block(2)
    gathered[PH_A2 - 1, :, cols(w)] = mlp_finish(2)
    gather_start(PH_A2)
    gather_forward(PH_A2)
    gather_finish(PH_A2)
    layer_norm(lambda row: gathered[PH_A2 - 1, row, :])
    y = matmul(lnbuf[...], k_final)
    for ww in range(W):
        ystage[ww] = y[ww * R:(ww + 1) * R, :].astype(BF16)

    def y_send_step(ww, carry):
        @pl.when(ww != w)
        def _():
            rcopy(ystage.at[ww], ybuf.at[w], y_send.at[ww], y_recv.at[w], dev(t, ww // 2, lax.rem(ww, 2))).start()

        @pl.when(ww == w)
        def _():
            ybuf[w] = ystage[ww]
        return carry

    lax.fori_loop(0, W, y_send_step, 0)

    def y_recv_step(ww, carry):
        @pl.when(ww != w)
        def _():
            rcopy(ystage.at[ww], ybuf.at[ww], y_send.at[ww], y_recv.at[ww], partner).wait()
        return carry

    lax.fori_loop(0, W, y_recv_step, 0)
    for ww in range(W):
        y_ref[:, ww * C:(ww + 1) * C] = ybuf[ww]

    for ph in range(NUM_PH):
        gather_drain(ph)
    for blk in range(3):
        qkv_drain(blk, blk // 2)
        mlp_drain(blk)
    for stage in range(2):
        attention_drain(stage)


def solution(mesh):
    n = mesh.shape['branch']

    def device_step(x, h, in_qkv, in_proj, in_up, in_down, tail_qkv, tail_proj, tail_up, tail_down, z_hint, z_out, w_final):
        R, D = x.shape[1:]
        heads_w = D // W // HD
        T = n // W
        M = W * R
        C = D // W
        FS = in_up.shape[-1] // W
        vmem = pl.BlockSpec(memory_space=pltpu.VMEM)
        hbm = pl.BlockSpec(memory_space=pl.ANY)
        dma = pltpu.SemaphoreType.DMA
        y = pl.pallas_call(
            functools.partial(kernel, n, heads_w),
            out_shape=jax.ShapeDtypeStruct((R, D), BF16),
            in_specs=[vmem] * 2 + [hbm] * 11,
            out_specs=vmem,
            scratch_shapes=[
                pltpu.VMEM((SLOTS, D, C), BF16),
                dma((SLOTS,)),
                pltpu.VMEM((W, 2, R, D), BF16),
                pltpu.VMEM((2, M, D), BF16),
                pltpu.VMEM((NUM_PH - 1, M, D), BF16),
                pltpu.VMEM((M, D), BF16),
                pltpu.VMEM((M, FS), BF16),
                pltpu.VMEM((3, 3, heads_w, M, HD), BF16),
                pltpu.VMEM((2, 3, T * M, HD), BF16),
                pltpu.VMEM((2, T * M, HD), BF16),
                pltpu.VMEM((3, 4, M, C), F32),
                pltpu.VMEM((3, 4, M, C), F32),
                pltpu.VMEM((3, 3, M, C), F32),
                pltpu.VMEM((3, 3, M, C), F32),
                pltpu.VMEM((3, M, C), F32),
                pltpu.VMEM((W, R, C), BF16),
                pltpu.VMEM((W, R, C), BF16),
                dma((NUM_PH, 7)), dma((NUM_PH, 7)),
                dma((3, 3, heads_w)), dma((2, T)),
                dma((2, T)), dma((3, heads_w)),
                dma((3, 4)), dma((3, 4)),
                dma((3, 3)), dma((3, 3)),
                dma((W,)), dma((W,)),
            ],
            compiler_params=pltpu.CompilerParams(collective_id=0, has_side_effects=True, vmem_limit_bytes=67043328),
        )(
            x[0], h[0], in_qkv[:, 0], in_proj[:, 0].reshape(2, D, D), in_up[:, 0], in_down[:, 0],
            tail_qkv, tail_proj.reshape(1, D, D), tail_up, tail_down, z_hint, z_out, w_final,
        )
        return y[None]

    act_spec = P('data', 'branch', None)
    return jax.shard_map(device_step, mesh=mesh, in_specs=(act_spec, act_spec) + (P(),) * 11, out_specs=act_spec, check_vma=False)
```

```python
import functools

import jax
import jax.numpy as jnp
from jax import lax
from jax.experimental import pallas as pl
from jax.experimental.pallas import tpu as pltpu
from jax.sharding import PartitionSpec as P

MESH = pl.DeviceIdType.MESH
F32 = jnp.float32
BF16 = jnp.bfloat16
LN_EPS = 1e-6
W = 8
HD = 128
SLOTS = 17

FAR_FIRST = (3, 1, 2, 0)

PH_H, PH_X, PH_C1, PH_U2, PH_O = 0, 1, 2, 3, 4
G_C0, G_O, G_U, G_C1, G_U2, G_A1, G_OT, G_UT = 0, 1, 3, 5, 6, 7, 8, 9
NUM_G = 10
G_ATT = (G_O, G_O + 1, G_OT)
G_MID = (G_U, G_U + 1, G_UT)
SH_C0, SH_U, SH_A1 = 0, 1, 4
NUM_SH = 5


def normalise(rows):
    centred = rows - jnp.mean(rows, axis=-1, keepdims=True)
    variance = jnp.mean(centred * centred, axis=-1, keepdims=True)
    return (centred * lax.rsqrt(variance + LN_EPS)).astype(BF16)


def add_rounded(a, b):
    return (a.astype(F32) + b.astype(F32)).astype(BF16)


def kernel(n, heads_w, x_ref, h_ref, in_qkv, in_proj, in_up, in_down, tail_qkv, tail_proj, tail_up, tail_down, z_hint, z_out, w_final,
           y_ref, wbuf, wsem, xs, xh, gathered, lnbuf, lnrow, hid, qkv_out, qkv_in, o_out, sum_out, sum_in, sum_own, row_out, row_in,
           ag_send, ag_recv, sh_send, sh_recv, qkv_send, qkv_recv, o_send, o_recv, hid_send, hid_recv, sum_send, sum_recv, row_send, row_recv):
    T = n // W
    R = x_ref.shape[0]
    D = x_ref.shape[1]
    M = W * R
    C = D // W
    FS = hid.shape[2] // 2
    NW1 = FS // C
    scale = HD ** -0.5 * 1.4426950408889634

    me = lax.axis_index('branch')
    if n == 128:
        c = lax.rem(me, 2)
        x0 = lax.rem(me // 2, 2)
        x1 = lax.rem(me // 4, 2)
        y0 = lax.rem(me // 8, 2)
        y1 = lax.rem(me // 16, 2)
        j = y0 * 2 + x0
        t = (me // 32) * 4 + y1 * 2 + x1
    else:
        c = lax.rem(me, 2)
        j = lax.rem(me, W) // 2
        t = me // W
    w = j * 2 + c

    def dev(tt, jj, cc):
        if n == 128:
            return (tt // 4) * 32 + lax.rem(tt // 2, 2) * 16 + (jj // 2) * 8 + lax.rem(tt, 2) * 4 + lax.rem(jj, 2) * 2 + cc
        return tt * W + jj * 2 + cc

    def near(r):
        return lax.rem(j // 2 + r // 2, 2) * 2 + lax.rem(lax.rem(j, 2) + lax.rem(r, 2), 2)

    def rcopy(src, dst, ssem, rsem, device):
        return pltpu.make_async_remote_copy(src_ref=src, dst_ref=dst, send_sem=ssem, recv_sem=rsem, device_id={'branch': device}, device_id_type=MESH)

    partner = dev(t, j, 1 - c)

    def cols(ww):
        return pl.ds(pl.multiple_of(ww * C, HD), C)

    def head_cols(ww, h):
        return pl.ds(pl.multiple_of(ww * C + h * HD, HD), HD)

    chunks = []

    def add(source):
        chunks.append(source)
        return len(chunks) - 1

    def columns_of(ref, start):
        return ref.at[:, pl.ds(pl.multiple_of(start, HD), C)]

    def add_qkv(ref):
        return [add(columns_of(ref, p * D + w * C)) for p in (1, 2, 0)][0]

    def add_up(ref):
        return [add(columns_of(ref, w * FS + i * C)) for i in range(NW1)][0]

    def add_slices(ref):
        return [add(columns_of(ref, (near(r) * 2 + c) * C)) for r in range(4)][0]

    def add_down(ref, starts):
        return [add(ref.at[pl.ds(pl.multiple_of(j * 2 * FS, 16), 2 * FS), pl.ds(pl.multiple_of(start, HD), C)]) for start in starts][0]

    qkv_refs = (in_qkv.at[0], in_qkv.at[1], tail_qkv.at[0])
    proj_refs = (in_proj.at[0], in_proj.at[1], tail_proj.at[0])
    up_refs = (in_up.at[0], in_up.at[1], tail_up.at[0])
    down_refs = (in_down.at[0], in_down.at[1], tail_down.at[0])
    k_qkv, k_proj, k_up, k_down = {}, {}, {}, {}
    k_hint = add_slices(z_hint)
    for b in (0, 1):
        k_qkv[b] = add_qkv(qkv_refs[b])
    for b in (0, 1):
        k_proj[b] = add_slices(proj_refs[b])
    for b in (1, 0):
        k_up[b] = add_up(up_refs[b])
    for b in (1, 0):
        k_down[b] = add_down(down_refs[b], [(near(r) * 2 + c) * C for r in FAR_FIRST])
    k_zout = add_slices(z_out.at[0])
    k_qkv[2] = add_qkv(qkv_refs[2])
    k_proj[2] = add_slices(proj_refs[2])
    k_up[2] = add_up(up_refs[2])
    k_down[2] = add_down(down_refs[2], [(4 * c + m) * C for m in range(4)])
    k_final = [add(columns_of(w_final, m * C)) for m in range(W)][0]

    def fetch(k):
        pltpu.make_async_copy(chunks[k], wbuf.at[k % SLOTS], wsem.at[k % SLOTS]).start()

    def ready(slot):
        pltpu.make_async_copy(columns_of(z_hint, 0), wbuf.at[slot], wsem.at[slot]).wait()

    def refill(first, count):
        for k in range(first, first + count):
            if k + SLOTS < len(chunks):
                fetch(k + SLOTS)

    for k in range(min(SLOTS, len(chunks))):
        fetch(k)

    barrier = pltpu.get_barrier_semaphore()

    def greet_group(ww, carry):
        @pl.when(ww != w)
        def _():
            pl.semaphore_signal(barrier, inc=1, device_id={'branch': dev(t, ww // 2, lax.rem(ww, 2))}, device_id_type=MESH)
        return carry

    def greet_tokens(tt, carry):
        @pl.when(tt != t)
        def _():
            pl.semaphore_signal(barrier, inc=1, device_id={'branch': dev(tt, j, c)}, device_id_type=MESH)
        return carry

    lax.fori_loop(0, W, greet_group, 0)
    lax.fori_loop(0, T, greet_tokens, 0)
    xs[PH_H, w] = h_ref[...]
    xs[PH_X, w] = x_ref[...]
    pl.semaphore_wait(barrier, W - 1 + T - 1)

    landing = {PH_C1: G_C1, PH_U2: G_U2}
    num_ph = PH_O + 3 * heads_w

    def att_phases(blk):
        return range(PH_O + blk * heads_w, PH_O + (blk + 1) * heads_w)

    def piece(ph, jj, cc):
        if ph in (PH_H, PH_X):
            return xs.at[ph, jj * 2 + cc]
        if ph >= PH_O:
            return gathered.at[G_ATT[(ph - PH_O) // heads_w], :, head_cols(jj * 2 + cc, (ph - PH_O) % heads_w)]
        return gathered.at[landing[ph], :, cols(jj * 2 + cc)]

    def gather_start(ph):
        own = piece(ph, j, c)
        for r in (3, 1, 2):
            rcopy(own, own, ag_send.at[ph, r], ag_recv.at[ph, r], dev(t, near(r), c)).start()
        if ph != PH_U2:
            rcopy(own, own, ag_send.at[ph, 0], ag_recv.at[ph, 0], partner).start()

    def gather_forward(ph):
        for r in (1, 2, 3):
            got = piece(ph, near(r), c)
            rcopy(got, got, ag_send.at[ph, r], ag_recv.at[ph, r], partner).wait_recv()
            rcopy(got, got, ag_send.at[ph, 3 + r], ag_recv.at[ph, 3 + r], partner).start()

    def gather_finish(ph):
        for r in range(4):
            got = piece(ph, near(r), 1 - c)
            s = 0 if r == 0 else 3 + r
            rcopy(got, got, ag_send.at[ph, s], ag_recv.at[ph, s], partner).wait_recv()

    def gather_drain(ph):
        for s in range(7) if ph != PH_U2 else (1, 2, 3):
            own = piece(ph, j, c)
            rcopy(own, own, ag_send.at[ph, s], ag_recv.at[ph, s], partner).wait_send()

    def layer_norm(load):
        for i in range(M // 16):
            lnbuf[i * 16:(i + 1) * 16, :] = normalise(load(slice(i * 16, (i + 1) * 16)).astype(F32))

    def matmul(lhs, k):
        ready(k % SLOTS)
        return jnp.dot(lhs, wbuf[k % SLOTS], preferred_element_type=F32)

    def shared_dots(lhs, first, dst, lo, hi):
        def slice_step(r, carry):
            slot = lax.rem(first + r, SLOTS)
            ready(slot)
            gathered[dst, :, cols(near(r) * 2 + c)] = jnp.dot(lhs[...], wbuf[slot], preferred_element_type=F32).astype(BF16)
            return carry

        lax.fori_loop(lo, hi, slice_step, 0)
        refill(first + lo, hi - lo)

    def hand_over(dst, sh, r):
        handed = gathered.at[dst, :, cols(near(r) * 2 + c)]
        rcopy(handed, handed, sh_send.at[sh, r], sh_recv.at[sh, r], partner).start()

    def shared_add(residual, dst, sh, awaited=None):
        for r in range(4):
            mine = cols(near(r) * 2 + c)
            if awaited is not None and r > 0:
                got = piece(awaited, near(r), c)
                rcopy(got, got, ag_send.at[awaited, r], ag_recv.at[awaited, r], partner).wait_recv()
            gathered[dst, :, mine] = add_rounded(residual[:, mine], gathered[dst, :, mine])
            hand_over(dst, sh, r)

    def shared_matmul(lhs, first, residual, dst, sh):
        def slice_step(r, carry):
            slot = lax.rem(first + r, SLOTS)
            mine = cols(near(r) * 2 + c)
            ready(slot)
            out = jnp.dot(lhs[...], wbuf[slot], preferred_element_type=F32).astype(BF16)
            gathered[dst, :, mine] = add_rounded(residual[:, mine], out)
            hand_over(dst, sh, r)
            return carry

        lax.fori_loop(0, 4, slice_step, 0)
        refill(first, 4)

    def shared_finish(dst, sh):
        for r in range(4):
            got = gathered.at[dst, :, cols(near(r) * 2 + 1 - c)]
            rcopy(got, got, sh_send.at[sh, r], sh_recv.at[sh, r], partner).wait_recv()

    def shared_drain(sh):
        for r in range(4):
            own = gathered.at[0, :, cols(w)]
            rcopy(own, own, sh_send.at[sh, r], sh_recv.at[sh, r], partner).wait_send()

    def owner(blk, h):
        if n == 128:
            return (1 - c if blk == 0 else 2 + c) * 4 + h + 1
        return blk % 2 * heads_w + h

    def qkv_block(blk, stage):
        first = k_qkv[blk]

        def part_step(i, carry):
            p = lax.rem(i + 1, 3)
            slot = lax.rem(first + i, SLOTS)
            ready(slot)
            out = jnp.dot(lnbuf[...], wbuf[slot], preferred_element_type=F32).astype(BF16)
            dst_rows = pl.ds(pl.multiple_of(t * M, M), M)
            for h in range(heads_w):
                qkv_out[blk, p, h] = out[:, h * HD:(h + 1) * HD]
            for h in range(heads_w):
                to = owner(blk, h)

                @pl.when(to != t)
                def _():
                    rcopy(qkv_out.at[blk, p, h], qkv_in.at[stage, p, dst_rows], qkv_send.at[blk, p, h], qkv_recv.at[stage, t], dev(to, j, c)).start()

                @pl.when(to == t)
                def _():
                    qkv_in[stage, p, dst_rows, :] = out[:, h * HD:(h + 1) * HD]
            return carry

        lax.fori_loop(0, 3, part_step, 0)
        refill(first, 3)

    def qkv_drain(blk, stage):
        for p in range(3):
            for h in range(heads_w):
                @pl.when(owner(blk, h) != t)
                def _():
                    rcopy(qkv_out.at[blk, p, h], qkv_in.at[stage, p, pl.ds(0, M)], qkv_send.at[blk, p, h], qkv_recv.at[stage, t], partner).wait_send()

    QB = min(512, T * M)
    QH = QB // 2
    if n == 128:
        last = jnp.logical_and(t // 4 == 2 + c, lax.rem(t, 4) > 0)
        first_blk = jnp.logical_and(t // 4 == 1 - c, lax.rem(t, 4) > 0)
        owns = (jnp.logical_or(first_blk, last), last)
        own_blk = t // 8
        own_head = jnp.maximum(lax.rem(t, 4) - 1, 0)
    else:
        owns = (t < 2 * heads_w, t < heads_w)
        own_blk = t // heads_w
        own_head = lax.rem(t, heads_w)

    def attention(stage):
        land = G_O + own_blk if stage == 0 else G_OT
        blk = own_blk if stage == 0 else 2

        @pl.when(owns[stage])
        def _():
            def arrive(tt, carry):
                @pl.when(tt != t)
                def _():
                    slab = qkv_in.at[stage, :, pl.ds(pl.multiple_of(tt * M, M), M)]
                    rcopy(slab, slab, o_send.at[stage, t], qkv_recv.at[stage, tt], partner).wait_recv()
                return carry

            lax.fori_loop(0, T, arrive, 0)

            def queries(i, carry):
                rows = [pl.ds(pl.multiple_of(i * QB + g * QH, QH), QH) for g in range(2)]
                scores = [lax.dot_general(qkv_in[stage, 0, row, :], qkv_in[stage, 1], (((1,), (1,)), ((), ())), preferred_element_type=F32) for row in rows]
                for row, s in zip(rows, scores):
                    e = jnp.exp2((s - jnp.max(s, axis=-1, keepdims=True)) * scale)
                    p = (e * (1.0 / jnp.sum(e, axis=-1, keepdims=True))).astype(BF16)
                    o_out[stage, row, :] = jnp.dot(p, qkv_in[stage, 2], preferred_element_type=F32).astype(BF16)
                for q in range(QB // M):
                    tt = i * (QB // M) + q
                    mine = pl.ds(pl.multiple_of(tt * M, M), M)
                    dst = gathered.at[land, :, head_cols(w, own_head)]

                    @pl.when(tt != t)
                    def _():
                        rcopy(o_out.at[stage, mine], dst, o_send.at[stage, tt], o_recv.at[blk, own_head], dev(tt, j, c)).start()

                    @pl.when(tt == t)
                    def _():
                        dst[...] = o_out[stage, mine, :]
                return carry

            lax.fori_loop(0, T * M // QB, queries, 0)

    def attention_drain(stage):
        @pl.when(owns[stage])
        def _():
            def left(tt, carry):
                @pl.when(tt != t)
                def _():
                    mine = o_out.at[stage, pl.ds(pl.multiple_of(tt * M, M), M)]
                    rcopy(mine, mine, o_send.at[stage, tt], o_recv.at[0, 0], partner).wait_send()
                return carry
            lax.fori_loop(0, T, left, 0)

    def attention_gather(blk):
        for h, ph in enumerate(att_phases(blk)):
            @pl.when(owner(blk, h) != t)
            def _():
                got = piece(ph, j, c)
                rcopy(got, got, o_send.at[0, t], o_recv.at[blk, h], partner).wait_recv()
            gather_start(ph)

    def proj_block(blk):
        residual = (xh.at[PH_X], gathered.at[G_C0], gathered.at[G_A1])[blk]
        for ph in att_phases(blk):
            gather_forward(ph)
        for ph in att_phases(blk):
            gather_finish(ph)
        shared_matmul(gathered.at[G_ATT[blk]], k_proj[blk], residual, G_MID[blk], SH_U + blk)

    def up_block(blk):
        shared_finish(G_MID[blk], SH_U + blk)
        layer_norm(lambda row: gathered[G_MID[blk], row, :])

        def up_step(i, carry):
            slot = lax.rem(k_up[blk] + i, SLOTS)
            ready(slot)
            out = jnp.dot(lnbuf[...], wbuf[slot], preferred_element_type=F32)
            mine = pl.ds(pl.multiple_of(c * FS + i * C, HD), C)
            hid[blk, :, mine] = jax.nn.gelu(out, approximate=True).astype(BF16)
            rcopy(hid.at[blk, :, mine], hid.at[blk, :, mine], hid_send.at[blk, i], hid_recv.at[blk, i], partner).start()
            return carry

        lax.fori_loop(0, NW1, up_step, 0)
        refill(k_up[blk], NW1)

    def hidden_ready(blk):
        for i in range(NW1):
            got = hid.at[blk, :, pl.ds(pl.multiple_of((1 - c) * FS + i * C, HD), C)]
            rcopy(got, got, hid_send.at[blk, i], hid_recv.at[blk, i], partner).wait_recv()

    def hidden_drain(blk):
        for i in range(NW1):
            got = hid.at[blk, :, pl.ds(pl.multiple_of(c * FS + i * C, HD), C)]
            rcopy(got, got, hid_send.at[blk, i], hid_recv.at[blk, i], partner).wait_send()

    def down_block(blk):
        hidden_ready(blk)
        for s, r in enumerate(FAR_FIRST):
            out = matmul(hid[blk], k_down[blk] + s)
            if r == 0:
                sum_own[blk] = out
            else:
                sum_out[blk, r - 1] = out
                rcopy(sum_out.at[blk, r - 1], sum_in.at[blk, r - 1], sum_send.at[blk, r - 1], sum_recv.at[blk, r - 1], dev(t, near(r), c)).start()
        refill(k_down[blk], 4)

    def down_finish(blk):
        total = sum_own[blk]
        for s in range(3):
            rcopy(sum_out.at[blk, s], sum_in.at[blk, s], sum_send.at[blk, s], sum_recv.at[blk, s], partner).wait_recv()
            total = total + sum_in[blk, s]
        return add_rounded(gathered[G_MID[blk], :, cols(w)], total.astype(BF16))

    def down_drain(blk):
        for s in range(3):
            rcopy(sum_out.at[blk, s], sum_in.at[blk, s], sum_send.at[blk, s], sum_recv.at[blk, s], partner).wait_send()

    def down_rows():
        def half_dot(m, core):
            part = pl.ds(pl.multiple_of(core * FS, HD), FS)
            return jnp.dot(hid[2, :, part], wbuf[(k_down[2] + m) % SLOTS, part, :], preferred_element_type=F32)

        for m in range(4):
            span = slice(m * C, (m + 1) * C)
            if m < 2:
                ready((k_down[2] + m) % SLOTS)
                row_out[:, span] = half_dot(m, c)
        hidden_ready(2)
        for m in range(4):
            span = slice(m * C, (m + 1) * C)
            row_out[:, span] = row_out[:, span] + half_dot(m, 1 - c) if m < 2 else matmul(hid[2], k_down[2] + m)
            for r in FAR_FIRST:
                for cc in ((c, 1 - c) if r else (1 - c,)):
                    to = near(r) * 2 + cc
                    out = row_out.at[pl.ds(pl.multiple_of(to * R, R), R), span]
                    rcopy(out, row_in.at[w, :, span], row_send.at[m, to], row_recv.at[m, w], dev(t, near(r), cc)).start()
        refill(k_down[2], 4)

    def rows_finish():
        def arrive(ww, carry):
            @pl.when(ww != w)
            def _():
                for m in range(4):
                    got = row_in.at[ww, :, m * C:(m + 1) * C]
                    rcopy(got, got, row_send.at[m, ww], row_recv.at[m, ww], partner).wait()
            return carry

        lax.fori_loop(0, W, arrive, 0)
        row_in[w] = row_out[pl.ds(pl.multiple_of(w * R, R), R), :]
        sums = []
        for cc in range(2):
            total = row_in[cc]
            for jj in range(1, 4):
                total = total + row_in[jj * 2 + cc]
            sums.append(total.astype(BF16))
        both = gathered[G_UT, pl.ds(pl.multiple_of(w // 2 * 2 * R, 2 * R), 2 * R), :].astype(F32)
        residual = jnp.where(c == 0, both[:R], both[R:])
        return (residual + jnp.concatenate(sums, axis=1).astype(F32)).astype(BF16)

    def unpack(ph):
        for i in range(M // 16):
            rows = [xs[ph, 16 // R * i + q].astype(F32) for q in range(16 // R)]
            xh[ph, i * 16:(i + 1) * 16, :] = jnp.concatenate(rows, axis=0).astype(BF16)

    gather_start(PH_H)
    gather_start(PH_X)
    gather_forward(PH_H)
    gather_finish(PH_H)
    unpack(PH_H)
    shared_dots(xh.at[PH_H], k_hint, G_C0, 0, 2)
    gather_forward(PH_X)
    shared_dots(xh.at[PH_H], k_hint, G_C0, 2, 4)
    gather_finish(PH_X)
    unpack(PH_X)
    shared_add(xh.at[PH_X], G_C0, SH_C0)
    layer_norm(lambda row: xh[PH_X, row, :])
    qkv_block(0, 0)
    shared_finish(G_C0, SH_C0)
    layer_norm(lambda row: gathered[G_C0, row, :])
    qkv_block(1, 0)
    attention(0)
    attention_gather(0)
    attention_gather(1)
    proj_block(0)
    proj_block(1)
    up_block(1)
    up_block(0)
    down_block(1)
    down_block(0)
    gathered[G_C1, :, cols(w)] = down_finish(1)
    gather_start(PH_C1)
    gather_forward(PH_C1)
    gathered[G_U2, :, cols(w)] = down_finish(0)
    gather_start(PH_U2)
    gather_finish(PH_C1)
    shared_dots(gathered.at[G_C1], k_zout, G_A1, 0, 4)
    shared_add(gathered.at[G_U2], G_A1, SH_A1, PH_U2)
    shared_finish(G_A1, SH_A1)
    layer_norm(lambda row: gathered[G_A1, row, :])
    qkv_block(2, 1)
    attention(1)
    attention_gather(2)
    proj_block(2)
    up_block(2)
    down_rows()
    lnrow[...] = normalise(rows_finish().astype(F32))

    def final_step(m, carry):
        slot = lax.rem(k_final + m, SLOTS)
        ready(slot)
        out = jnp.dot(lnrow[...], wbuf[slot], preferred_element_type=F32)
        y_ref[:, pl.ds(pl.multiple_of(m * C, HD), C)] = out.astype(BF16)
        return carry

    lax.fori_loop(0, W, final_step, 0)

    for ph in range(num_ph):
        gather_drain(ph)
    for sh in range(NUM_SH):
        shared_drain(sh)
    for blk in range(3):
        qkv_drain(blk, blk // 2)
        hidden_drain(blk)
    for blk in range(2):
        down_drain(blk)
    for stage in range(2):
        attention_drain(stage)


def solution(mesh):
    n = mesh.shape['branch']

    def device_step(x, h, in_qkv, in_proj, in_up, in_down, tail_qkv, tail_proj, tail_up, tail_down, z_hint, z_out, w_final):
        R, D = x.shape[1:]
        heads_w = D // W // HD
        T = n // W
        M = W * R
        C = D // W
        FS = in_up.shape[-1] // W
        vmem = pl.BlockSpec(memory_space=pltpu.VMEM)
        hbm = pl.BlockSpec(memory_space=pl.ANY)
        dma = pltpu.SemaphoreType.DMA
        y = pl.pallas_call(
            functools.partial(kernel, n, heads_w),
            out_shape=jax.ShapeDtypeStruct((R, D), BF16),
            in_specs=[vmem] * 2 + [hbm] * 11,
            out_specs=vmem,
            scratch_shapes=[
                pltpu.VMEM((SLOTS, D, C), BF16),
                dma((SLOTS,)),
                pltpu.VMEM((2, W, R, D), BF16),
                pltpu.VMEM((2, M, D), BF16),
                pltpu.VMEM((NUM_G, M, D), BF16),
                pltpu.VMEM((M, D), BF16),
                pltpu.VMEM((R, D), BF16),
                pltpu.VMEM((3, M, 2 * FS), BF16),
                pltpu.VMEM((3, 3, heads_w, M, HD), BF16),
                pltpu.VMEM((2, 3, T * M, HD), BF16),
                pltpu.VMEM((2, T * M, HD), BF16),
                pltpu.VMEM((2, 3, M, C), F32),
                pltpu.VMEM((2, 3, M, C), F32),
                pltpu.VMEM((2, M, C), F32),
                pltpu.VMEM((M, D // 2), F32),
                pltpu.VMEM((W, R, D // 2), F32),
                dma((PH_O + 3 * heads_w, 7)), dma((PH_O + 3 * heads_w, 7)),
                dma((NUM_SH, 4)), dma((NUM_SH, 4)),
                dma((3, 3, heads_w)), dma((2, T)),
                dma((2, T)), dma((3, heads_w)),
                dma((3, FS // C)), dma((3, FS // C)),
                dma((2, 3)), dma((2, 3)),
                dma((4, W)), dma((4, W)),
            ],
            compiler_params=pltpu.CompilerParams(collective_id=0, has_side_effects=True, vmem_limit_bytes=67043328),
        )(
            x[0], h[0], in_qkv[:, 0], in_proj[:, 0].reshape(2, D, D), in_up[:, 0], in_down[:, 0],
            tail_qkv, tail_proj.reshape(1, D, D), tail_up, tail_down, z_hint, z_out, w_final,
        )
        return y[None]

    act_spec = P('data', 'branch', None)
    return jax.shard_map(device_step, mesh=mesh, in_specs=(act_spec, act_spec) + (P(),) * 11, out_specs=act_spec, check_vma=False)
```

```python
import functools

import jax
import jax.numpy as jnp
from jax import lax
from jax.experimental import pallas as pl
from jax.experimental.pallas import tpu as pltpu
from jax.sharding import PartitionSpec as P

MESH = pl.DeviceIdType.MESH
F32 = jnp.float32
BF16 = jnp.bfloat16
LN_EPS = 1e-6
W = 8
HD = 128
SLOTS = 17

FAR_FIRST = (3, 1, 2, 0)

PH_H, PH_X, PH_O, PH_C1, PH_OT, PH_U2 = 0, 1, 2, 4, 5, 6
NUM_PH = 7
G_C0, G_O, G_U, G_C1, G_U2, G_A1, G_OT, G_UT = 0, 1, 3, 5, 6, 7, 8, 9
NUM_G = 10
PH_ATT = (PH_O, PH_O + 1, PH_OT)
G_ATT = (G_O, G_O + 1, G_OT)
G_MID = (G_U, G_U + 1, G_UT)
SH_C0, SH_U, SH_A1 = 0, 1, 4
NUM_SH = 5


def normalise(rows):
    centred = rows - jnp.mean(rows, axis=-1, keepdims=True)
    variance = jnp.mean(centred * centred, axis=-1, keepdims=True)
    return (centred * lax.rsqrt(variance + LN_EPS)).astype(BF16)


def add_rounded(a, b):
    return (a.astype(F32) + b.astype(F32)).astype(BF16)


def kernel(n, heads_w, x_ref, h_ref, in_qkv, in_proj, in_up, in_down, tail_qkv, tail_proj, tail_up, tail_down, z_hint, z_out, w_final,
           y_ref, wbuf, wsem, xs, xh, gathered, lnbuf, lnrow, hid, qkv_out, qkv_in, o_out, sum_out, sum_in, sum_own, row_out, row_in,
           ag_send, ag_recv, sh_send, sh_recv, qkv_send, qkv_recv, o_send, o_recv, hid_send, hid_recv, sum_send, sum_recv, row_send, row_recv):
    T = n // W
    R = x_ref.shape[0]
    D = x_ref.shape[1]
    M = W * R
    C = D // W
    FS = hid.shape[2] // 2
    NW1 = FS // C
    scale = HD ** -0.5 * 1.4426950408889634

    me = lax.axis_index('branch')
    if n == 128:
        c = lax.rem(me, 2)
        x0 = lax.rem(me // 2, 2)
        x1 = lax.rem(me // 4, 2)
        y0 = lax.rem(me // 8, 2)
        y1 = lax.rem(me // 16, 2)
        j = y0 * 2 + x0
        t = (me // 32) * 4 + y1 * 2 + x1
        spread = T // 2
    else:
        c = lax.rem(me, 2)
        j = lax.rem(me, W) // 2
        t = me // W
        spread = 0
    w = j * 2 + c

    def dev(tt, jj, cc):
        if n == 128:
            return (tt // 4) * 32 + lax.rem(tt // 2, 2) * 16 + (jj // 2) * 8 + lax.rem(tt, 2) * 4 + lax.rem(jj, 2) * 2 + cc
        return tt * W + jj * 2 + cc

    def near(r):
        return lax.rem(j // 2 + r // 2, 2) * 2 + lax.rem(lax.rem(j, 2) + lax.rem(r, 2), 2)

    def rcopy(src, dst, ssem, rsem, device):
        return pltpu.make_async_remote_copy(src_ref=src, dst_ref=dst, send_sem=ssem, recv_sem=rsem, device_id={'branch': device}, device_id_type=MESH)

    partner = dev(t, j, 1 - c)

    def cols(ww):
        return pl.ds(pl.multiple_of(ww * C, HD), C)

    chunks = []

    def add(source):
        chunks.append(source)
        return len(chunks) - 1

    def columns_of(ref, start):
        return ref.at[:, pl.ds(pl.multiple_of(start, HD), C)]

    def add_qkv(ref):
        return [add(columns_of(ref, p * D + w * C)) for p in (1, 2, 0)][0]

    def add_up(ref):
        return [add(columns_of(ref, w * FS + i * C)) for i in range(NW1)][0]

    def add_slices(ref):
        return [add(columns_of(ref, (near(r) * 2 + c) * C)) for r in range(4)][0]

    def add_down(ref, starts):
        return [add(ref.at[pl.ds(pl.multiple_of(j * 2 * FS, 16), 2 * FS), pl.ds(pl.multiple_of(start, HD), C)]) for start in starts][0]

    qkv_refs = (in_qkv.at[0], in_qkv.at[1], tail_qkv.at[0])
    proj_refs = (in_proj.at[0], in_proj.at[1], tail_proj.at[0])
    up_refs = (in_up.at[0], in_up.at[1], tail_up.at[0])
    down_refs = (in_down.at[0], in_down.at[1], tail_down.at[0])
    k_qkv, k_proj, k_up, k_down = {}, {}, {}, {}
    k_hint = add_slices(z_hint)
    for b in (0, 1):
        k_qkv[b] = add_qkv(qkv_refs[b])
    for b in (0, 1):
        k_proj[b] = add_slices(proj_refs[b])
    for b in (1, 0):
        k_up[b] = add_up(up_refs[b])
        k_down[b] = add_down(down_refs[b], [(near(r) * 2 + c) * C for r in FAR_FIRST])
    k_zout = add_slices(z_out.at[0])
    k_qkv[2] = add_qkv(qkv_refs[2])
    k_proj[2] = add_slices(proj_refs[2])
    k_up[2] = add_up(up_refs[2])
    k_down[2] = add_down(down_refs[2], [(4 * c + m) * C for m in range(4)])
    k_final = [add(columns_of(w_final, m * C)) for m in range(W)][0]

    def fetch(k):
        pltpu.make_async_copy(chunks[k], wbuf.at[k % SLOTS], wsem.at[k % SLOTS]).start()

    def ready(slot):
        pltpu.make_async_copy(columns_of(z_hint, 0), wbuf.at[slot], wsem.at[slot]).wait()

    def refill(first, count):
        for k in range(first, first + count):
            if k + SLOTS < len(chunks):
                fetch(k + SLOTS)

    for k in range(min(SLOTS, len(chunks))):
        fetch(k)

    barrier = pltpu.get_barrier_semaphore()

    def greet_group(ww, carry):
        @pl.when(ww != w)
        def _():
            pl.semaphore_signal(barrier, inc=1, device_id={'branch': dev(t, ww // 2, lax.rem(ww, 2))}, device_id_type=MESH)
        return carry

    def greet_tokens(tt, carry):
        @pl.when(tt != t)
        def _():
            pl.semaphore_signal(barrier, inc=1, device_id={'branch': dev(tt, j, c)}, device_id_type=MESH)
        return carry

    lax.fori_loop(0, W, greet_group, 0)
    lax.fori_loop(0, T, greet_tokens, 0)
    xs[PH_H, w] = h_ref[...]
    xs[PH_X, w] = x_ref[...]
    pl.semaphore_wait(barrier, W - 1 + T - 1)

    landing = {PH_O: G_O, PH_O + 1: G_O + 1, PH_C1: G_C1, PH_OT: G_OT, PH_U2: G_U2}

    def piece(ph, jj, cc):
        if ph in (PH_H, PH_X):
            return xs.at[ph, jj * 2 + cc]
        return gathered.at[landing[ph], :, cols(jj * 2 + cc)]

    def gather_start(ph):
        own = piece(ph, j, c)
        for r in (3, 1, 2):
            rcopy(own, own, ag_send.at[ph, r], ag_recv.at[ph, r], dev(t, near(r), c)).start()
        if ph != PH_U2:
            rcopy(own, own, ag_send.at[ph, 0], ag_recv.at[ph, 0], partner).start()

    def gather_forward(ph):
        for r in (1, 2, 3):
            got = piece(ph, near(r), c)
            rcopy(got, got, ag_send.at[ph, r], ag_recv.at[ph, r], partner).wait_recv()
            rcopy(got, got, ag_send.at[ph, 3 + r], ag_recv.at[ph, 3 + r], partner).start()

    def gather_finish(ph):
        for r in range(4):
            got = piece(ph, near(r), 1 - c)
            s = 0 if r == 0 else 3 + r
            rcopy(got, got, ag_send.at[ph, s], ag_recv.at[ph, s], partner).wait_recv()

    def gather_drain(ph):
        for s in range(7) if ph != PH_U2 else (1, 2, 3):
            own = piece(ph, j, c)
            rcopy(own, own, ag_send.at[ph, s], ag_recv.at[ph, s], partner).wait_send()

    def layer_norm(load):
        for i in range(M // 16):
            lnbuf[i * 16:(i + 1) * 16, :] = normalise(load(slice(i * 16, (i + 1) * 16)).astype(F32))

    def matmul(lhs, k):
        ready(k % SLOTS)
        return jnp.dot(lhs, wbuf[k % SLOTS], preferred_element_type=F32)

    def shared_matmul(lhs, first, residual, dst, sh, awaited=None):
        def slice_step(r, carry):
            slot = lax.rem(first + r, SLOTS)
            mine = cols(near(r) * 2 + c)
            ready(slot)
            out = jnp.dot(lhs[...], wbuf[slot], preferred_element_type=F32).astype(BF16)
            if awaited is not None:
                @pl.when(r > 0)
                def _():
                    got = piece(awaited, near(r), c)
                    rcopy(got, got, ag_send.at[awaited, r], ag_recv.at[awaited, r], partner).wait_recv()
            gathered[dst, :, mine] = add_rounded(residual[:, mine], out)
            handed = gathered.at[dst, :, mine]
            rcopy(handed, handed, sh_send.at[sh, r], sh_recv.at[sh, r], partner).start()
            return carry

        lax.fori_loop(0, 4, slice_step, 0)
        refill(first, 4)

    def shared_dots(lhs, first, dst, lo, hi):
        def slice_step(r, carry):
            slot = lax.rem(first + r, SLOTS)
            ready(slot)
            gathered[dst, :, cols(near(r) * 2 + c)] = jnp.dot(lhs[...], wbuf[slot], preferred_element_type=F32).astype(BF16)
            return carry

        lax.fori_loop(lo, hi, slice_step, 0)
        refill(first + lo, hi - lo)

    def shared_add(residual, dst, sh):
        for r in range(4):
            mine = cols(near(r) * 2 + c)
            gathered[dst, :, mine] = add_rounded(residual[:, mine], gathered[dst, :, mine])
            handed = gathered.at[dst, :, mine]
            rcopy(handed, handed, sh_send.at[sh, r], sh_recv.at[sh, r], partner).start()

    def shared_finish(dst, sh):
        for r in range(4):
            got = gathered.at[dst, :, cols(near(r) * 2 + 1 - c)]
            rcopy(got, got, sh_send.at[sh, r], sh_recv.at[sh, r], partner).wait_recv()

    def shared_drain(sh):
        for r in range(4):
            own = gathered.at[0, :, cols(w)]
            rcopy(own, own, sh_send.at[sh, r], sh_recv.at[sh, r], partner).wait_send()

    def owner(blk, h):
        return (blk % 2) * heads_w + h + spread * c

    def qkv_block(blk, stage):
        first = k_qkv[blk]

        def part_step(i, carry):
            p = lax.rem(i + 1, 3)
            slot = lax.rem(first + i, SLOTS)
            ready(slot)
            out = jnp.dot(lnbuf[...], wbuf[slot], preferred_element_type=F32).astype(BF16)
            dst_rows = pl.ds(pl.multiple_of(t * M, M), M)
            for h in range(heads_w):
                qkv_out[blk, p, h] = out[:, h * HD:(h + 1) * HD]
            for h in range(heads_w):
                to = owner(blk, h)

                @pl.when(to != t)
                def _():
                    rcopy(qkv_out.at[blk, p, h], qkv_in.at[stage, p, dst_rows], qkv_send.at[blk, p, h], qkv_recv.at[stage, t], dev(to, j, c)).start()

                @pl.when(to == t)
                def _():
                    qkv_in[stage, p, dst_rows, :] = out[:, h * HD:(h + 1) * HD]
            return carry

        lax.fori_loop(0, 3, part_step, 0)
        refill(first, 3)

    def qkv_drain(blk, stage):
        for p in range(3):
            for h in range(heads_w):
                @pl.when(owner(blk, h) != t)
                def _():
                    rcopy(qkv_out.at[blk, p, h], qkv_in.at[stage, p, pl.ds(0, M)], qkv_send.at[blk, p, h], qkv_recv.at[stage, t], partner).wait_send()

    QB = min(512, T * M)
    QH = QB // 2
    place = t - spread * c
    owns = (jnp.logical_and(place >= 0, place < 2 * heads_w), jnp.logical_and(place >= 0, place < heads_w))
    own_blk = place // heads_w
    own_head = lax.rem(place, heads_w)

    def attention(stage):
        land = G_O + own_blk if stage == 0 else G_OT
        blk = own_blk if stage == 0 else 2

        @pl.when(owns[stage])
        def _():
            def arrive(tt, carry):
                @pl.when(tt != t)
                def _():
                    slab = qkv_in.at[stage, :, pl.ds(pl.multiple_of(tt * M, M), M)]
                    rcopy(slab, slab, o_send.at[stage, t], qkv_recv.at[stage, tt], partner).wait_recv()
                return carry

            lax.fori_loop(0, T, arrive, 0)

            def queries(i, carry):
                rows = [pl.ds(pl.multiple_of(i * QB + g * QH, QH), QH) for g in range(2)]
                scores = [lax.dot_general(qkv_in[stage, 0, row, :], qkv_in[stage, 1], (((1,), (1,)), ((), ())), preferred_element_type=F32) for row in rows]
                for row, s in zip(rows, scores):
                    e = jnp.exp2((s - jnp.max(s, axis=-1, keepdims=True)) * scale)
                    p = (e * (1.0 / jnp.sum(e, axis=-1, keepdims=True))).astype(BF16)
                    o_out[stage, row, :] = jnp.dot(p, qkv_in[stage, 2], preferred_element_type=F32).astype(BF16)
                for q in range(QB // M):
                    tt = i * (QB // M) + q
                    mine = pl.ds(pl.multiple_of(tt * M, M), M)
                    dst = gathered.at[land, :, pl.ds(pl.multiple_of(w * C + own_head * HD, HD), HD)]

                    @pl.when(tt != t)
                    def _():
                        rcopy(o_out.at[stage, mine], dst, o_send.at[stage, tt], o_recv.at[blk, own_head], dev(tt, j, c)).start()

                    @pl.when(tt == t)
                    def _():
                        dst[...] = o_out[stage, mine, :]
                return carry

            lax.fori_loop(0, T * M // QB, queries, 0)

    def attention_drain(stage):
        @pl.when(owns[stage])
        def _():
            def left(tt, carry):
                @pl.when(tt != t)
                def _():
                    mine = o_out.at[stage, pl.ds(pl.multiple_of(tt * M, M), M)]
                    rcopy(mine, mine, o_send.at[stage, tt], o_recv.at[0, 0], partner).wait_send()
                return carry
            lax.fori_loop(0, T, left, 0)

    def attention_gather(blk):
        for h in range(heads_w):
            @pl.when(owner(blk, h) != t)
            def _():
                got = gathered.at[G_ATT[blk], :, pl.ds(pl.multiple_of(w * C + h * HD, HD), HD)]
                rcopy(got, got, o_send.at[0, t], o_recv.at[blk, h], partner).wait_recv()
        gather_start(PH_ATT[blk])

    def proj_block(blk):
        residual = (xh.at[PH_X], gathered.at[G_C0], gathered.at[G_A1])[blk]
        gather_forward(PH_ATT[blk])
        gather_finish(PH_ATT[blk])
        shared_matmul(gathered.at[G_ATT[blk]], k_proj[blk], residual, G_MID[blk], SH_U + blk)

    def up_block(blk):
        shared_finish(G_MID[blk], SH_U + blk)
        layer_norm(lambda row: gathered[G_MID[blk], row, :])

        def up_step(i, carry):
            slot = lax.rem(k_up[blk] + i, SLOTS)
            ready(slot)
            out = jnp.dot(lnbuf[...], wbuf[slot], preferred_element_type=F32)
            mine = pl.ds(pl.multiple_of(c * FS + i * C, HD), C)
            hid[blk, :, mine] = jax.nn.gelu(out, approximate=True).astype(BF16)
            rcopy(hid.at[blk, :, mine], hid.at[blk, :, mine], hid_send.at[blk, i], hid_recv.at[blk, i], partner).start()
            return carry

        lax.fori_loop(0, NW1, up_step, 0)
        refill(k_up[blk], NW1)

    def hidden_ready(blk):
        for i in range(NW1):
            got = hid.at[blk, :, pl.ds(pl.multiple_of((1 - c) * FS + i * C, HD), C)]
            rcopy(got, got, hid_send.at[blk, i], hid_recv.at[blk, i], partner).wait_recv()

    def hidden_drain(blk):
        for i in range(NW1):
            got = hid.at[blk, :, pl.ds(pl.multiple_of(c * FS + i * C, HD), C)]
            rcopy(got, got, hid_send.at[blk, i], hid_recv.at[blk, i], partner).wait_send()

    def down_block(blk):
        hidden_ready(blk)
        for s, r in enumerate(FAR_FIRST):
            out = matmul(hid[blk], k_down[blk] + s)
            if r == 0:
                sum_own[blk] = out
            else:
                sum_out[blk, r - 1] = out
                rcopy(sum_out.at[blk, r - 1], sum_in.at[blk, r - 1], sum_send.at[blk, r - 1], sum_recv.at[blk, r - 1], dev(t, near(r), c)).start()
        refill(k_down[blk], 4)

    def down_finish(blk):
        total = sum_own[blk]
        for s in range(3):
            rcopy(sum_out.at[blk, s], sum_in.at[blk, s], sum_send.at[blk, s], sum_recv.at[blk, s], partner).wait_recv()
            total = total + sum_in[blk, s]
        return add_rounded(gathered[G_MID[blk], :, cols(w)], total.astype(BF16))

    def down_drain(blk):
        for s in range(3):
            rcopy(sum_out.at[blk, s], sum_in.at[blk, s], sum_send.at[blk, s], sum_recv.at[blk, s], partner).wait_send()

    def down_rows():
        hidden_ready(2)
        for half in range(2):
            for m in (2 * half, 2 * half + 1):
                row_out[:, m * C:(m + 1) * C] = matmul(hid[2], k_down[2] + m)
            span = pl.ds(half * 2 * C, 2 * C)
            for r in FAR_FIRST:
                for cc in ((c, 1 - c) if r else (1 - c,)):
                    to = near(r) * 2 + cc
                    out = row_out.at[pl.ds(pl.multiple_of(to * R, R), R), span]
                    rcopy(out, row_in.at[w, :, span], row_send.at[half, to], row_recv.at[half, w], dev(t, near(r), cc)).start()

    def rows_finish():
        def arrive(ww, carry):
            @pl.when(ww != w)
            def _():
                for half in range(2):
                    span = pl.ds(half * 2 * C, 2 * C)
                    got = row_in.at[ww, :, span]
                    rcopy(got, got, row_send.at[half, ww], row_recv.at[half, ww], partner).wait()
            return carry

        lax.fori_loop(0, W, arrive, 0)
        row_in[w] = row_out[pl.ds(pl.multiple_of(w * R, R), R), :]
        sums = []
        for cc in range(2):
            total = row_in[cc]
            for jj in range(1, 4):
                total = total + row_in[jj * 2 + cc]
            sums.append(total.astype(BF16))
        both = gathered[G_UT, pl.ds(pl.multiple_of(w // 2 * 2 * R, 2 * R), 2 * R), :].astype(F32)
        residual = jnp.where(c == 0, both[:R], both[R:])
        return (residual + jnp.concatenate(sums, axis=1).astype(F32)).astype(BF16)

    def unpack(ph):
        for i in range(M // 16):
            rows = [xs[ph, 16 // R * i + q].astype(F32) for q in range(16 // R)]
            xh[ph, i * 16:(i + 1) * 16, :] = jnp.concatenate(rows, axis=0).astype(BF16)

    gather_start(PH_H)
    gather_start(PH_X)
    gather_forward(PH_H)
    gather_finish(PH_H)
    unpack(PH_H)
    shared_dots(xh.at[PH_H], k_hint, G_C0, 0, 2)
    gather_forward(PH_X)
    shared_dots(xh.at[PH_H], k_hint, G_C0, 2, 4)
    gather_finish(PH_X)
    unpack(PH_X)
    shared_add(xh.at[PH_X], G_C0, SH_C0)
    layer_norm(lambda row: xh[PH_X, row, :])
    qkv_block(0, 0)
    shared_finish(G_C0, SH_C0)
    layer_norm(lambda row: gathered[G_C0, row, :])
    qkv_block(1, 0)
    attention(0)
    attention_gather(0)
    attention_gather(1)
    proj_block(0)
    proj_block(1)
    up_block(1)
    down_block(1)
    up_block(0)
    down_block(0)
    gathered[G_C1, :, cols(w)] = down_finish(1)
    gather_start(PH_C1)
    gather_forward(PH_C1)
    gathered[G_U2, :, cols(w)] = down_finish(0)
    gather_start(PH_U2)
    gather_finish(PH_C1)
    shared_matmul(gathered.at[G_C1], k_zout, gathered.at[G_U2], G_A1, SH_A1, PH_U2)
    shared_finish(G_A1, SH_A1)
    layer_norm(lambda row: gathered[G_A1, row, :])
    qkv_block(2, 1)
    attention(1)
    attention_gather(2)
    proj_block(2)
    up_block(2)
    down_rows()
    lnrow[...] = normalise(rows_finish().astype(F32))

    def final_step(m, carry):
        slot = lax.rem(k_final + m, SLOTS)
        ready(slot)
        out = jnp.dot(lnrow[...], wbuf[slot], preferred_element_type=F32)
        y_ref[:, pl.ds(pl.multiple_of(m * C, HD), C)] = out.astype(BF16)
        return carry

    lax.fori_loop(0, W, final_step, 0)

    for ph in range(NUM_PH):
        gather_drain(ph)
    for sh in range(NUM_SH):
        shared_drain(sh)
    for blk in range(3):
        qkv_drain(blk, blk // 2)
        hidden_drain(blk)
    for blk in range(2):
        down_drain(blk)
    for stage in range(2):
        attention_drain(stage)


def solution(mesh):
    n = mesh.shape['branch']

    def device_step(x, h, in_qkv, in_proj, in_up, in_down, tail_qkv, tail_proj, tail_up, tail_down, z_hint, z_out, w_final):
        R, D = x.shape[1:]
        heads_w = D // W // HD
        T = n // W
        M = W * R
        C = D // W
        FS = in_up.shape[-1] // W
        vmem = pl.BlockSpec(memory_space=pltpu.VMEM)
        hbm = pl.BlockSpec(memory_space=pl.ANY)
        dma = pltpu.SemaphoreType.DMA
        y = pl.pallas_call(
            functools.partial(kernel, n, heads_w),
            out_shape=jax.ShapeDtypeStruct((R, D), BF16),
            in_specs=[vmem] * 2 + [hbm] * 11,
            out_specs=vmem,
            scratch_shapes=[
                pltpu.VMEM((SLOTS, D, C), BF16),
                dma((SLOTS,)),
                pltpu.VMEM((2, W, R, D), BF16),
                pltpu.VMEM((2, M, D), BF16),
                pltpu.VMEM((NUM_G, M, D), BF16),
                pltpu.VMEM((M, D), BF16),
                pltpu.VMEM((R, D), BF16),
                pltpu.VMEM((3, M, 2 * FS), BF16),
                pltpu.VMEM((3, 3, heads_w, M, HD), BF16),
                pltpu.VMEM((2, 3, T * M, HD), BF16),
                pltpu.VMEM((2, T * M, HD), BF16),
                pltpu.VMEM((2, 3, M, C), F32),
                pltpu.VMEM((2, 3, M, C), F32),
                pltpu.VMEM((2, M, C), F32),
                pltpu.VMEM((M, D // 2), F32),
                pltpu.VMEM((W, R, D // 2), F32),
                dma((NUM_PH, 7)), dma((NUM_PH, 7)),
                dma((NUM_SH, 4)), dma((NUM_SH, 4)),
                dma((3, 3, heads_w)), dma((2, T)),
                dma((2, T)), dma((3, heads_w)),
                dma((3, FS // C)), dma((3, FS // C)),
                dma((2, 3)), dma((2, 3)),
                dma((2, W)), dma((2, W)),
            ],
            compiler_params=pltpu.CompilerParams(collective_id=0, has_side_effects=True, vmem_limit_bytes=67043328),
        )(
            x[0], h[0], in_qkv[:, 0], in_proj[:, 0].reshape(2, D, D), in_up[:, 0], in_down[:, 0],
            tail_qkv, tail_proj.reshape(1, D, D), tail_up, tail_down, z_hint, z_out, w_final,
        )
        return y[None]

    act_spec = P('data', 'branch', None)
    return jax.shard_map(device_step, mesh=mesh, in_specs=(act_spec, act_spec) + (P(),) * 11, out_specs=act_spec, check_vma=False)
```
